32 devices in a mesh: pairs: 8 (over z, y), cols: 4 (over x, core).
Axes of the slice: x: 2, y: 2, z: 4, core: 2. Of those that a mesh axis runs over, the one named last changes fastest.
Arguments:
- amplitudes: bfloat16 [64, 256, 256], P('pairs', 'cols'), may hold values from -6 to 6
- pno_counts: int32 [64], P('pairs'), may hold values from 96 to 256
- fock_blocks: bfloat16 [64, 256, 256], P('pairs'), may hold values from -1 to 5, as said below
- exchange_blocks: bfloat16 [64, 256, 256], P('pairs', 'cols'), may hold values from -6 to 6
- intersections: bfloat16 [64, 32, 256, 256], P('pairs', None, 'cols'), may hold values from -0.375 to 0.375
- partners: int32 [64, 32], P('pairs'), may hold values from 0 to 63, as said below
- couplings: float32 [64, 32], P('pairs'), may hold values from -3 to 3
Outputs:
- residual_blocks: bfloat16 [64, 256, 256], P('pairs', 'cols')
The draws below stay inside these ranges and needn't reach their ends.
Inputs may be any that keep to these rules, and one draw needn't show every extreme that they name: `partners`: within the coupling lists of one aligned block of 8 pairs, at most 64 entries name pairs of any one aligned block of 8 pairs, and exactly 64 do for some block. `fock_blocks`: each block is symmetric.
All inputs are finite; a program needn't handle non-finite values.
Results may differ from the reference program's by a relative error of at most 0.0022.
Values may be sent and summed in bfloat16 or wider, within the bound.
No kernel may reach another device: no remote copies, remote signals or barrier semaphores. Data moves between devices by JAX's collectives and lax.ppermute only.
A program may use at most 128 MiB of HBM per device.

```python
import math
import jax
import jax.numpy as jnp
from jax import lax

PNO = 256
CPL = 32
PAIR_DEV = 8
NPAIRS = 64
N_PAIRS = 8


def draw_fock_blocks(key, part):
    total_pairs = PAIR_DEV * N_PAIRS
    first_key, second_key = jax.random.split(key)
    noise = jnp.clip(jax.random.normal(first_key, (total_pairs, PNO, PNO), jnp.float32), -3.0, 3.0) * 0.12
    symmetric = noise + jnp.swapaxes(noise, 1, 2)
    levels = jnp.exp(jax.random.uniform(second_key, (total_pairs, PNO), jnp.float32, 0.0, math.log(4.0)))
    return (symmetric + levels[:, :, None] * jnp.eye(PNO, dtype=jnp.float32)[None]).astype(jnp.bfloat16)


def draw_partners(key, part):
    slot_count = 2 * PAIR_DEV * CPL // N_PAIRS
    wanted_count = PAIR_DEV * CPL
    entries = N_PAIRS * slot_count

    def one_device(device_key):
        first_key, second_key, third_key, fourth_key = jax.random.split(device_key, 4)
        owner_pool = jnp.arange(entries, dtype=jnp.int32) // slot_count
        favored = jax.random.randint(first_key, (), 0, N_PAIRS).astype(jnp.int32)
        ranking = jax.random.permutation(second_key, entries).astype(jnp.int32)
        scores = jnp.where(owner_pool == favored, -1 - jnp.arange(entries, dtype=jnp.int32), ranking)
        chosen = owner_pool[jnp.argsort(scores, stable=True)[:wanted_count]]
        chosen = jax.random.permutation(third_key, chosen)
        within = jax.random.randint(fourth_key, (wanted_count,), 0, PAIR_DEV).astype(jnp.int32)
        return (chosen * PAIR_DEV + within).reshape(PAIR_DEV, CPL)
    device_keys = jax.random.split(key, N_PAIRS)
    return jax.vmap(one_device)(device_keys).reshape(PAIR_DEV * N_PAIRS, CPL).astype(jnp.int32)


def plant(drawn, own_key, low, largest):
    spot = [jax.random.randint(jax.random.fold_in(own_key, axis), (), 0, length) for axis, length in enumerate(drawn.shape)]
    longest = drawn.shape.index(max(drawn.shape))
    beside = spot[:longest] + [(spot[longest] + 1) % drawn.shape[longest]] + spot[longest + 1:]
    return drawn.at[tuple(spot)].set(low).at[tuple(beside)].set(largest)


def steps_of(key, extent, shards, least, high):
    loudness = 1.0
    for dim, parts in shards:
        draws = jax.random.uniform(jax.random.fold_in(jax.random.fold_in(key, 6), dim), (parts,), jnp.float32, least / len(shards), high / len(shards))
        loudness = loudness * jnp.repeat(jnp.exp(draws), extent[dim] // parts).reshape((-1,) + (1,) * (len(extent) - 1 - dim))
    return loudness


def gaussian(key, extent, scale, bound, pieces=(), kind=jnp.bfloat16):
    values = jax.random.normal(key, extent, jnp.float32) * scale
    if len(pieces) > 0:
        values = steps_of(key, extent, pieces, -0.22, 0.18) * values
    return jnp.clip(values, min=-bound, max=bound).astype(kind)


def setup_inputs(seed: int = 0) -> dict:
    arg_keys = jax.random.split(jax.random.key(seed), 8)
    amplitudes = gaussian(arg_keys[0], (NPAIRS, PNO, PNO), 1.0, 6.0, ((0, 8), (1, 4)))
    pno_counts = plant(jax.random.randint(arg_keys[1], (NPAIRS,), PNO * 3 // 8, PNO + 1), jax.random.fold_in(arg_keys[1], 1), PNO * 3 // 8, PNO).astype(jnp.int32)
    fock_blocks = draw_fock_blocks(jax.random.fold_in(arg_keys[7], 71), 0)
    exchange_blocks = gaussian(arg_keys[3], (NPAIRS, PNO, PNO), 1.0, 6.0, ((0, 8), (1, 4)))
    intersections = gaussian(arg_keys[4], (NPAIRS, CPL, PNO, PNO), PNO ** -0.5, 0.375, ((0, 8), (2, 4)))
    partners = draw_partners(jax.random.fold_in(arg_keys[7], 71), 0)
    couplings = gaussian(arg_keys[6], (NPAIRS, CPL), 0.5, 3.0, ((0, 8),), jnp.float32)
    return {"amplitudes": amplitudes, "pno_counts": pno_counts, "fock_blocks": fock_blocks, "exchange_blocks": exchange_blocks, "intersections": intersections, "partners": partners, "couplings": couplings}


def reference(amplitudes, pno_counts, fock_blocks, exchange_blocks, intersections, partners, couplings):
    inside = jnp.arange(PNO, dtype=jnp.int32)[None, :] < pno_counts[:, None]
    both = inside[:, :, None] & inside[:, None, :]
    masked = jnp.where(both, amplitudes, jnp.zeros_like(amplitudes))

    def one_pair(inputs):
        own, fock_one, exch_one, over_one, partner_ids, weights, keep = inputs
        total = exch_one.astype(jnp.float32)
        total = total + jnp.dot(fock_one, own, preferred_element_type=jnp.float32)
        total = total + jnp.dot(own, fock_one, preferred_element_type=jnp.float32)
        for slot_index in range(CPL):
            partner_block = masked[partner_ids[slot_index]]
            projected = jnp.dot(partner_block, over_one[slot_index], preferred_element_type=jnp.float32).astype(jnp.bfloat16)
            total = total + weights[slot_index] * jnp.dot(over_one[slot_index].T, projected, preferred_element_type=jnp.float32)
        return jnp.where(keep, total, jnp.zeros_like(total)).astype(jnp.bfloat16)

    return lax.map(one_pair, (masked, fock_blocks, exchange_blocks, intersections, partners, couplings, both))
```

```python
import functools
import jax
import jax.numpy as jnp
from jax import lax
from jax.experimental import pallas as pl
from jax.experimental.pallas import tpu as pltpu
from jax.sharding import PartitionSpec as P

GROUP = 4
CHUNKS = 4
RING_MAX = 8


def coupled_kernel(
    first, last, group, ways, own_pairs,
    slot_ref, weight_ref, info_ref, *refs,
):
    refs = list(refs)
    near = [refs.pop(0) for _ in range(group)]
    far = [refs.pop(0) for _ in range(group)]
    pieces = [refs.pop(0) for _ in range(ways)]
    if first:
        exch = [refs.pop(0) for _ in range(ways)]
        fock_ref, own_near, own_far = refs.pop(0), refs.pop(0), refs.pop(0)
    else:
        acc_ref = refs.pop(0)
    out_ref = refs.pop(0)
    whole, proj, total = refs
    share = pieces[0].shape[2]
    half = ways // 2
    pair, step = pl.program_id(0), pl.program_id(1)

    width = total.shape[0]

    def block(k):
        return info_ref[1 + 2 * own_pairs + k]

    def joined(ref):
        return ref[...].reshape(width, width)

    order = list(range(0, ways, 2)) + list(range(1, ways, 2))

    def contribution(left_near, left_far, right):
        for side, ks in ((left_near, order[:half]), (left_far, order[half:])):
            prod = jnp.dot(side, right, preferred_element_type=jnp.float32).astype(jnp.bfloat16)
            for n, k in enumerate(ks):
                proj[block(k)] = prod[n * share:(n + 1) * share]

    @pl.when(step == 0)
    def _():
        if first:
            for k in range(ways):
                proj[block(k)] = exch[k][0, 0]
            base = joined(proj).astype(jnp.float32)
            for side, ks in ((own_near, order[:half]), (own_far, order[half:])):
                for n, k in enumerate(ks):
                    whole[block(k)] = side[0, n * share:(n + 1) * share]
            own = joined(whole)
            fock = fock_ref[0]
            base = base + jnp.dot(fock, own, preferred_element_type=jnp.float32)
            total[...] = base + jnp.dot(own, fock, preferred_element_type=jnp.float32)
        else:
            total[...] = acc_ref[0]

    for g in range(group):
        for k in range(ways):
            whole[block(k)] = pieces[k][0, g]
        right = joined(whole)
        contribution(near[g][0], far[g][0], right)
        term = lax.dot_general(
            right, joined(proj), (((0,), (0,)), ((), ())), preferred_element_type=jnp.float32
        )
        weight = weight_ref[pair * (pl.num_programs(1) * group) + step * group + g]
        total[...] += weight * term

    @pl.when(step == pl.num_programs(1) - 1)
    def _():
        if last:
            count = info_ref[1 + pair]
            row = lax.broadcasted_iota(jnp.int32, (width, width), 0)
            col = lax.broadcasted_iota(jnp.int32, (width, width), 1)
            keep = (row < count) & (col < count)
            out_ref[0] = jnp.where(keep, total[...], 0.0).astype(jnp.bfloat16)
        else:
            out_ref[0] = total[...]


def run_chunk(
    start, size, first, last, near, far, own_pieces, got, slots, weights, info, acc, exch, fock
):
    own_pairs = got[0][0].shape[0]
    ways = len(got) + 1
    half_rows, width = near.shape[1], near.shape[2]
    share = own_pieces.shape[2]
    group = GROUP
    steps = size // group
    slot = lax.slice_in_dim(slots, start, start + size, axis=1).reshape(-1)
    weight = lax.slice_in_dim(weights, start, start + size, axis=1).reshape(-1)

    def partner_spec(g):
        return pl.BlockSpec(
            (1, half_rows, width),
            lambda m, s, sl, we, inf: (sl[m * (steps * group) + s * group + g], 0, 0),
        )

    in_specs = [partner_spec(g) for g in range(group)] * 2
    operands = [near] * group + [far] * group
    in_specs.append(pl.BlockSpec(
        (1, group, share, width),
        lambda m, s, sl, we, inf: (inf[0] * own_pairs + m, start // group + s, 0, 0),
    ))
    operands.append(own_pieces)
    for piece, offset in got:
        in_specs.append(pl.BlockSpec(
            (1, group, share, width),
            functools.partial(lambda o, m, s, sl, we, inf: (m, o + s, 0, 0), offset // group)))
        operands.append(piece)
    if first:
        in_specs.append(pl.BlockSpec(
            (1, 1, share, width), lambda m, s, sl, we, inf: (inf[0] * own_pairs + m, 0, 0, 0)))
        operands.append(exch[:, None])
        for piece, _ in got:
            in_specs.append(pl.BlockSpec(
                (1, 1, share, width),
                functools.partial(lambda o, m, s, sl, we, inf: (m, o, 0, 0), piece.shape[1] - 1)))
            operands.append(piece)
        in_specs.append(pl.BlockSpec(
            (1, width, width), lambda m, s, sl, we, inf: (inf[0] * own_pairs + m, 0, 0)))
        operands.append(fock)
        for array in (near, far):
            in_specs.append(pl.BlockSpec(
                (1, half_rows, width), lambda m, s, sl, we, inf: (inf[1 + own_pairs + m], 0, 0)))
            operands.append(array)
    else:
        in_specs.append(pl.BlockSpec((1, width, width), lambda m, s, sl, we, inf: (m, 0, 0)))
        operands.append(acc)
    out_type = jnp.bfloat16 if last else jnp.float32
    units = own_pairs * size
    return pl.pallas_call(
        functools.partial(coupled_kernel, first, last, group, ways, own_pairs),
        out_shape=jax.ShapeDtypeStruct((own_pairs, width, width), out_type),
        grid_spec=pltpu.PrefetchScalarGridSpec(
            num_scalar_prefetch=3,
            grid=(own_pairs, steps),
            in_specs=in_specs,
            out_specs=pl.BlockSpec((1, width, width), lambda m, s, sl, we, inf: (m, 0, 0)),
            scratch_shapes=[
                pltpu.VMEM((ways, share, width), jnp.bfloat16),
                pltpu.VMEM((ways, share, width), jnp.bfloat16),
                pltpu.VMEM((width, width), jnp.float32),
            ],
        ),
        cost_estimate=pl.CostEstimate(
            flops=units * 4 * width**3, bytes_accessed=units * 4 * width**2, transcendentals=0),
        compiler_params=pltpu.CompilerParams(dimension_semantics=("arbitrary", "arbitrary")),
        name="coupled",
    )(slot, weight, info, *operands)


def gather_pairs(half, count):
    me = lax.axis_index("pairs")
    if count > RING_MAX or count % 2:
        return lax.all_gather(half, "pairs", axis=0, tiled=True), lambda block: block
    order = list(range(0, count, 2)) + list(range(count - 1, 0, -2))
    ahead = [(order[i], order[(i + 1) % count]) for i in range(count)]
    behind = [(b, a) for a, b in ahead]
    mid = half.shape[0] // 2
    forward = backward = half
    from_ahead, from_behind = [], []
    for _ in range(1, count // 2):
        forward = lax.ppermute(forward, "pairs", ahead)
        backward = lax.ppermute(backward, "pairs", behind)
        from_behind.append(forward)
        from_ahead.append(backward)
    low = lax.ppermute(forward[:mid], "pairs", ahead)
    high = lax.ppermute(backward[mid:], "pairs", behind)
    whole = jnp.concatenate([half] + from_ahead + [low, high] + from_behind[::-1], axis=0)

    def place_of(block):
        return jnp.where(block % 2 == 0, block // 2, count - 1 - block // 2)

    return whole, lambda block: (place_of(block) - place_of(me) + count) % count


def shards(
    columns, amplitudes, pno_counts, fock_blocks, exchange_blocks, intersections, partners, couplings
):
    local_pairs, share, width = amplitudes.shape
    ways, count = columns, lax.axis_size("pairs")
    slots_per_pair = partners.shape[1]
    own_pairs = local_pairs // ways
    column = lax.axis_index("cols")
    row_keep = column * share + jnp.arange(share, dtype=jnp.int32)[None, :] < pno_counts[:, None]
    col_keep = jnp.arange(width, dtype=jnp.int32)[None, :] < pno_counts[:, None]
    keep = row_keep[:, :, None] & col_keep[:, None, :]
    masked = jnp.where(keep, amplitudes, jnp.zeros_like(amplitudes))

    def swap(array, k):
        return lax.ppermute(array, "cols", [(c, c ^ k) for c in range(ways)])

    half = jnp.concatenate(
        [masked] + [swap(masked, k) for k in range(2, ways, 2)], axis=1)

    size = slots_per_pair // CHUNKS

    def moved(k, start, stop):
        begin = (column ^ k) * own_pairs
        piece = lax.dynamic_slice(
            intersections, (begin, start, 0, 0), (own_pairs, stop - start, share, width))
        if start == 0:
            extra = lax.dynamic_slice_in_dim(exchange_blocks, begin, own_pairs, 0)
            piece = jnp.concatenate([piece, extra[:, None]], axis=1)
        return swap(piece, k)

    beside = moved(1, 0, slots_per_pair)
    got = []
    for chunk in range(CHUNKS):
        start = chunk * size
        got.append([(beside, start)] + [
            (moved(k, start, start + size), 0) for k in range(2, ways)])

    near, place = gather_pairs(half, count)
    far = swap(near, 1)

    begin = column * own_pairs
    own_partners = lax.dynamic_slice_in_dim(partners, begin, own_pairs, 0)
    weights = lax.dynamic_slice_in_dim(couplings, begin, own_pairs, 0)
    slots = place(own_partners // local_pairs) * local_pairs + own_partners % local_pairs
    own_counts = lax.dynamic_slice_in_dim(pno_counts, begin, own_pairs, 0)
    own_slots = place(lax.axis_index("pairs")) * local_pairs + begin + jnp.arange(own_pairs, dtype=jnp.int32)
    blocks = column ^ jnp.arange(ways, dtype=jnp.int32)
    info = jnp.concatenate([column[None].astype(jnp.int32), own_counts, own_slots, blocks])

    acc = None
    for chunk in range(CHUNKS):
        acc = run_chunk(
            chunk * size, size, chunk == 0, chunk == CHUNKS - 1, near, far, intersections,
            got[chunk], slots, weights, info, acc, exchange_blocks, fock_blocks)
    return lax.all_to_all(acc, "cols", split_axis=1, concat_axis=0, tiled=True)


def solution(mesh):
    in_specs = (
        P("pairs", "cols", None),
        P("pairs"),
        P("pairs", None, None),
        P("pairs", "cols", None),
        P("pairs", None, "cols", None),
        P("pairs", None),
        P("pairs", None),
    )
    out_specs = P("pairs", "cols", None)
    ways = mesh.shape["cols"]
    body = functools.partial(shards, ways)
    return jax.shard_map(body, mesh=mesh, in_specs=in_specs, out_specs=out_specs, check_vma=False)
```

```python
import functools
import jax
import jax.numpy as jnp
from jax import lax
from jax.experimental import pallas as pl
from jax.experimental.pallas import tpu as pltpu
from jax.sharding import PartitionSpec as P

CHUNKS = (24, 29)
RING_MAX = 8


def coupled_kernel(
    first, last, size, start, stride, offsets,
    slot_ref, weight_ref, info_ref, near, far, own, *refs,
):
    refs = list(refs)
    ways = len(offsets) + 1
    own_pairs = (info_ref.shape[0] - 1 - ways) // 2
    got = [refs.pop(0) for _ in range(ways - 1)]
    if first:
        exch, fock = refs.pop(0), refs.pop(0)
    else:
        acc = refs.pop(0)
    outs = [refs.pop(0) for _ in range(ways if last else 1)]
    left, right, proj, left_sem, right_sem = (refs.pop(0) for _ in range(5))
    group, share, width = right.shape[1], right.shape[3], right.shape[4]
    order = list(range(0, ways, 2)) + list(range(1, ways, 2))
    rounds = size // group
    column = info_ref[0]

    def block(k):
        return info_ref[1 + 2 * own_pairs + k]

    def fetch_partner(slot, place, sem):
        pltpu.make_async_copy(near.at[slot], place.at[0], sem).start()
        pltpu.make_async_copy(far.at[slot], place.at[1], sem).start()

    def fetch(r, _):
        m, q = lax.div(r, rounds), lax.rem(r, rounds) * group
        for g in range(group):
            fetch_partner(slot_ref[m * stride + start + q + g], left.at[r, g], left_sem.at[r])
        pltpu.make_async_copy(
            own.at[column * own_pairs + m, pl.ds(start + q, group)],
            right.at[r, :, block(0)], right_sem.at[r]).start()
        for k in range(1, ways):
            pltpu.make_async_copy(
                got[k - 1].at[m, pl.ds(offsets[k - 1] + q, group)],
                right.at[r, :, block(k)], right_sem.at[r]).start()
        return 0

    if first:
        base, mine, whole, base_sem, mine_sem, whole_sem = refs
        for m in range(own_pairs):
            pltpu.make_async_copy(
                fock.at[column * own_pairs + m], whole.at[m], whole_sem.at[m]).start()
            fetch_partner(info_ref[1 + own_pairs + m], mine.at[m], mine_sem.at[m])
            pltpu.make_async_copy(
                exch.at[column * own_pairs + m], base.at[m, block(0)], base_sem.at[m]).start()
            for k in range(1, ways):
                pltpu.make_async_copy(
                    got[k - 1].at[m, got[k - 1].shape[1] - 1], base.at[m, block(k)], base_sem.at[m]
                ).start()
    else:
        whole, whole_sem = refs
        for m in range(own_pairs):
            pltpu.make_async_copy(acc.at[m], whole.at[m], whole_sem.at[m]).start()
    lax.fori_loop(0, own_pairs * rounds, fetch, 0)

    def ready(ref, sem, i):
        pltpu.make_async_copy(ref.at[i], ref.at[i], sem.at[i]).wait()

    def arranged(rows, g):
        for n, k in enumerate(order):
            proj[g, block(k)] = rows[n * share:(n + 1) * share]

    for m in range(own_pairs):
        ready(whole, whole_sem, m)
        total = whole if last else outs[0]
        if first:
            ready(mine, mine_sem, m)
            ready(base, base_sem, m)
            arranged(mine[m].reshape(width, width), 0)
            diagonal = whole[m]
            block_own = proj[0].reshape(width, width)
            sums = base[m].reshape(width, width).astype(jnp.float32)
            sums = sums + jnp.dot(diagonal, block_own, preferred_element_type=jnp.float32)
            total[m] = sums + jnp.dot(block_own, diagonal, preferred_element_type=jnp.float32)
        elif not last:
            total[m] = whole[m]

        def body(n, _):
            r = m * rounds + n
            ready(left, left_sem, r)
            ready(right, right_sem, r)
            for g in range(group):
                prod = jnp.dot(
                    left[r, g].reshape(width, width), right[r, g].reshape(width, width),
                    preferred_element_type=jnp.float32)
                arranged(prod.astype(jnp.bfloat16), g)
            added = None
            for g in range(group):
                term = lax.dot_general(
                    right[r, g].reshape(width, width), proj[g].reshape(width, width),
                    (((0,), (0,)), ((), ())), preferred_element_type=jnp.float32)
                term = weight_ref[m * stride + start + n * group + g] * term
                added = term if added is None else added + term
            total[m] = total[m] + added
            return 0

        lax.fori_loop(0, rounds, body, 0)
        if last:
            count = info_ref[1 + m]
            row = lax.broadcasted_iota(jnp.int32, (width, width), 0)
            col = lax.broadcasted_iota(jnp.int32, (width, width), 1)
            keep = (row < count) & (col < count)
            total[m] = jnp.where(keep, total[m], 0.0)
            for k in range(ways):
                rows = pl.ds(pl.multiple_of(block(k) * share, share), share)
                outs[k][m] = total[m, rows, :].astype(jnp.bfloat16)


def run_chunk(
    start, size, first, last, near, far, own_pieces, got, slots, weights, info, acc, exch, fock
):
    own_pairs = got[0][0].shape[0]
    ways = len(got) + 1
    width = near.shape[2]
    share = own_pieces.shape[2]
    units = own_pairs * size
    anywhere = pl.BlockSpec(memory_space=pl.ANY)
    operands = [near, far, own_pieces] + [piece for piece, _ in got]
    operands += [exch, fock] if first else [acc]
    inside = pl.BlockSpec(memory_space=pltpu.VMEM)
    if last:
        out_shape = [jax.ShapeDtypeStruct((own_pairs, share, width), jnp.bfloat16)] * ways
        out_specs = [inside] * ways
    else:
        out_shape = jax.ShapeDtypeStruct((own_pairs, width, width), jnp.float32)
        out_specs = inside
    group = max(g for g in (1, 2, 3, 4, 5) if size % g == 0)
    rounds = units // group
    scratch = [
        pltpu.VMEM((rounds, group, 2, width // 2, width), jnp.bfloat16),
        pltpu.VMEM((rounds, group, ways, share, width), jnp.bfloat16),
        pltpu.VMEM((group, ways, share, width), jnp.bfloat16),
        pltpu.SemaphoreType.DMA((rounds,)),
        pltpu.SemaphoreType.DMA((rounds,)),
    ]
    pair_sems = pltpu.SemaphoreType.DMA((own_pairs,))
    if first:
        scratch += [
            pltpu.VMEM((own_pairs, ways, share, width), jnp.bfloat16),
            pltpu.VMEM((own_pairs, 2, width // 2, width), jnp.bfloat16),
            pltpu.VMEM((own_pairs, width, width), jnp.bfloat16),
            pair_sems, pair_sems, pair_sems,
        ]
    else:
        scratch += [pltpu.VMEM((own_pairs, width, width), jnp.float32), pair_sems]
    stride = slots.shape[0] // own_pairs
    return pl.pallas_call(
        functools.partial(
            coupled_kernel, first, last, size, start, stride, tuple(o for _, o in got)),
        out_shape=out_shape,
        grid_spec=pltpu.PrefetchScalarGridSpec(
            num_scalar_prefetch=3,
            grid=(),
            in_specs=[anywhere] * len(operands),
            out_specs=out_specs,
            scratch_shapes=scratch,
        ),
        cost_estimate=pl.CostEstimate(
            flops=units * 4 * width**3, bytes_accessed=units * 4 * width**2, transcendentals=0),
        name="coupled",
    )(slots, weights, info, *operands)


def gather_pairs(half, count):
    me = lax.axis_index("pairs")
    if count > RING_MAX or count % 2:
        return lax.all_gather(half, "pairs", axis=0, tiled=True), lambda block: block
    order = list(range(0, count, 2)) + list(range(count - 1, 0, -2))
    ahead = [(order[i], order[(i + 1) % count]) for i in range(count)]
    behind = [(b, a) for a, b in ahead]
    mid = half.shape[0] // 2
    forward = backward = half
    from_ahead, from_behind = [], []
    for _ in range(1, count // 2):
        forward = lax.ppermute(forward, "pairs", ahead)
        backward = lax.ppermute(backward, "pairs", behind)
        from_behind.append(forward)
        from_ahead.append(backward)
    low = lax.ppermute(forward[:mid], "pairs", ahead)
    high = lax.ppermute(backward[mid:], "pairs", behind)
    whole = jnp.concatenate([half] + from_ahead + [low, high] + from_behind[::-1], axis=0)

    def place_of(block):
        return jnp.where(block % 2 == 0, block // 2, count - 1 - block // 2)

    return whole, lambda block: (place_of(block) - place_of(me) + count) % count


def chunk_bounds(length):
    cuts = [0] + [length * c // 32 for c in CHUNKS] + [length]
    return list(zip(cuts, cuts[1:]))


def shards(
    columns, amplitudes, pno_counts, fock_blocks, exchange_blocks, intersections, partners, couplings
):
    local_pairs, share, width = amplitudes.shape
    ways, count = columns, lax.axis_size("pairs")
    slots_per_pair = partners.shape[1]
    own_pairs = local_pairs // ways
    column = lax.axis_index("cols")

    def swap(array, k):
        return lax.ppermute(array, "cols", [(c, c ^ k) for c in range(ways)])

    col_keep = jnp.arange(width, dtype=jnp.int32)[None, :] < pno_counts[:, None]

    def masked(array, k):
        row = (column ^ k) * share + jnp.arange(share, dtype=jnp.int32)
        keep = (row[None, :] < pno_counts[:, None])[:, :, None] & col_keep[:, None, :]
        return jnp.where(keep, array, jnp.zeros_like(array))

    parts = [masked(amplitudes, 0)]
    parts += [masked(swap(amplitudes, k), k) for k in range(2, ways, 2)]
    half = jnp.concatenate(parts, axis=1)
    bounds = chunk_bounds(slots_per_pair)

    def moved(k, start, stop):
        begin = (column ^ k) * own_pairs
        piece = lax.dynamic_slice(
            intersections, (begin, start, 0, 0), (own_pairs, stop - start, share, width))
        if start == 0:
            extra = lax.dynamic_slice_in_dim(exchange_blocks, begin, own_pairs, 0)
            piece = jnp.concatenate([piece, extra[:, None]], axis=1)
        return swap(piece, k)

    beside = moved(1, 0, slots_per_pair)
    got = []
    for start, stop in bounds:
        got.append([(beside, start)] + [
            (moved(k, start, stop), 0) for k in range(2, ways)])

    near, place = gather_pairs(half, count)
    far = swap(near, 1)

    begin = column * own_pairs
    own_partners = lax.dynamic_slice_in_dim(partners, begin, own_pairs, 0)
    weights = lax.dynamic_slice_in_dim(couplings, begin, own_pairs, 0)
    slots = place(own_partners // local_pairs) * local_pairs + own_partners % local_pairs
    own_counts = lax.dynamic_slice_in_dim(pno_counts, begin, own_pairs, 0)
    own_slots = place(lax.axis_index("pairs")) * local_pairs + begin + jnp.arange(own_pairs, dtype=jnp.int32)
    blocks = column ^ jnp.arange(ways, dtype=jnp.int32)
    info = jnp.concatenate([column[None].astype(jnp.int32), own_counts, own_slots, blocks])

    acc = None
    for n, (start, stop) in enumerate(bounds):
        acc = run_chunk(
            start, stop - start, n == 0, n == len(bounds) - 1, near, far, intersections,
            got[n], slots.reshape(-1), weights.reshape(-1), info, acc, exchange_blocks, fock_blocks)
    arrived = [acc[0]] + [swap(acc[k], k) for k in range(1, ways)]
    spots = blocks[:, None, None, None]
    shared = arrived[0][None]
    for k in range(1, ways):
        shared = jnp.where(spots == k, arrived[k][None], shared)
    return shared.reshape(local_pairs, share, width)


def solution(mesh):
    in_specs = (
        P("pairs", "cols", None),
        P("pairs"),
        P("pairs", None, None),
        P("pairs", "cols", None),
        P("pairs", None, "cols", None),
        P("pairs", None),
        P("pairs", None),
    )
    out_specs = P("pairs", "cols", None)
    ways = mesh.shape["cols"]
    body = functools.partial(shards, ways)
    return jax.shard_map(body, mesh=mesh, in_specs=in_specs, out_specs=out_specs, check_vma=False)
```

```python
import functools
import jax
import jax.numpy as jnp
from jax import lax
from jax.experimental import pallas as pl
from jax.experimental.pallas import tpu as pltpu
from jax.sharding import PartitionSpec as P

CHUNKS = (24, 29)
RING_MAX = 8
VMEM_LIMIT = 60 * 2**20


def coupled_kernel(
    first, last, size, after, start, stride, offsets, own_pairs,
    slots, weights, info, near, far, own, *refs,
):
    refs = list(refs)
    ways = len(offsets) + 1
    got = [refs.pop(0) for _ in range(ways - 1)]
    if first:
        exch, fock = refs.pop(0), refs.pop(0)
    else:
        acc = refs.pop(0)
    ready_left = refs.pop(0) if last else None
    outs = [refs.pop(0) for _ in range(ways if last else 1)]
    ahead = refs.pop(0) if after else None
    slot_ref, weight_ref, info_ref, scalar_sem = (refs.pop(0) for _ in range(4))
    left, right, proj, left_sem, right_sem = (refs.pop(0) for _ in range(5))
    ahead_sem = refs.pop(0) if after else None
    group, share, width = right.shape[1], right.shape[3], right.shape[4]
    order = list(range(0, ways, 2)) + list(range(1, ways, 2))
    rounds = size // group
    column = lax.axis_index("cols")
    scalars = [
        pltpu.make_async_copy(source, target, scalar_sem.at[i])
        for i, (source, target) in enumerate(
            ((slots, slot_ref), (weights, weight_ref), (info, info_ref)))
    ]
    for copy in scalars:
        copy.start()

    def block(k):
        return column ^ k

    def fetch_partner(slot, place, sem):
        pltpu.make_async_copy(near.at[slot], place.at[0], sem).start()
        pltpu.make_async_copy(far.at[slot], place.at[1], sem).start()

    def fetch_pieces(r, _):
        m, q = lax.div(r, rounds), lax.rem(r, rounds) * group
        pltpu.make_async_copy(
            own.at[column * own_pairs + m, pl.ds(start + q, group)],
            right.at[r, :, block(0)], right_sem.at[r]).start()
        for k in range(1, ways):
            pltpu.make_async_copy(
                got[k - 1].at[m, pl.ds(offsets[k - 1] + q, group)],
                right.at[r, :, block(k)], right_sem.at[r]).start()
        if last:
            pltpu.make_async_copy(
                ready_left.at[pl.ds(r * group, group)], left.at[r], left_sem.at[r]).start()
        return 0

    def fetch_partners(r):
        m, q = lax.div(r, rounds), lax.rem(r, rounds) * group
        for g in range(group):
            fetch_partner(slot_ref[m * stride + start + q + g], left.at[r, g], left_sem.at[r])
        return 0

    if first:
        base, mine, whole, base_sem, mine_sem, whole_sem = refs
        for m in range(own_pairs):
            pltpu.make_async_copy(
                fock.at[column * own_pairs + m], whole.at[m], whole_sem.at[m]).start()
            pltpu.make_async_copy(
                exch.at[column * own_pairs + m], base.at[m, block(0)], base_sem.at[m]).start()
            for k in range(1, ways):
                pltpu.make_async_copy(
                    got[k - 1].at[m, got[k - 1].shape[1] - 1], base.at[m, block(k)], base_sem.at[m]
                ).start()
    else:
        whole, whole_sem = refs
        for m in range(own_pairs):
            pltpu.make_async_copy(acc.at[m], whole.at[m], whole_sem.at[m]).start()

    def fetch(r, _):
        fetch_pieces(r, 0)
        return fetch_partners(r)

    if last:
        lax.fori_loop(0, own_pairs * rounds, fetch_pieces, 0)
    for copy in scalars:
        copy.wait()
    if first:
        for m in range(own_pairs):
            fetch_partner(info_ref[own_pairs + m], mine.at[m], mine_sem.at[m])
    if not last:
        lax.fori_loop(0, own_pairs * rounds, fetch, 0)
    for u in range(own_pairs * after):
        fetch_partner(
            slot_ref[u // after * stride + start + size + u % after], ahead.at[u], ahead_sem)

    def ready(ref, sem, i):
        pltpu.make_async_copy(ref.at[i], ref.at[i], sem.at[i]).wait()

    def arranged(rows, g):
        for n, k in enumerate(order):
            proj[g, block(k)] = rows[n * share:(n + 1) * share]

    for m in range(own_pairs):
        ready(whole, whole_sem, m)
        total = whole if last else outs[0]
        if first:
            ready(mine, mine_sem, m)
            ready(base, base_sem, m)
            arranged(mine[m].reshape(width, width), 0)
            diagonal = whole[m]
            block_own = proj[0].reshape(width, width)
            sums = base[m].reshape(width, width).astype(jnp.float32)
            sums = sums + jnp.dot(diagonal, block_own, preferred_element_type=jnp.float32)
            total[m] = sums + jnp.dot(block_own, diagonal, preferred_element_type=jnp.float32)
        elif not last:
            total[m] = whole[m]

        def body(n, _):
            r = m * rounds + n
            ready(left, left_sem, r)
            ready(right, right_sem, r)
            for g in range(group):
                prod = jnp.dot(
                    left[r, g].reshape(width, width), right[r, g].reshape(width, width),
                    preferred_element_type=jnp.float32)
                arranged(prod.astype(jnp.bfloat16), g)
            added = None
            for g in range(group):
                term = lax.dot_general(
                    right[r, g].reshape(width, width), proj[g].reshape(width, width),
                    (((0,), (0,)), ((), ())), preferred_element_type=jnp.float32)
                term = weight_ref[m * stride + start + n * group + g] * term
                added = term if added is None else added + term
            total[m] = total[m] + added
            return 0

        lax.fori_loop(0, rounds, body, 0)
        if last:
            count = info_ref[m]
            row = lax.broadcasted_iota(jnp.int32, (width, width), 0)
            col = lax.broadcasted_iota(jnp.int32, (width, width), 1)
            keep = (row < count) & (col < count)
            total[m] = jnp.where(keep, total[m], 0.0)
            for k in range(ways):
                rows = pl.ds(pl.multiple_of(block(k) * share, share), share)
                outs[k][m] = total[m, rows, :].astype(jnp.bfloat16)
    if after:
        pltpu.make_async_copy(ahead, ahead, ahead_sem).wait()


def run_chunk(
    start, size, after, first, last, ready_left, near, far, own_pieces, got, slots, weights, info, acc, exch, fock
):
    own_pairs = got[0][0].shape[0]
    ways = len(got) + 1
    width = near.shape[2]
    share = own_pieces.shape[2]
    units = own_pairs * size
    anywhere = pl.BlockSpec(memory_space=pl.ANY)
    operands = [slots, weights, info, near, far, own_pieces] + [piece for piece, _ in got]
    operands += [exch, fock] if first else [acc]
    if last:
        operands.append(ready_left)
    inside = pl.BlockSpec(memory_space=pltpu.VMEM)
    if last:
        out_shape = [jax.ShapeDtypeStruct((own_pairs, share, width), jnp.bfloat16)] * ways
        out_specs = [inside] * ways
    else:
        out_shape = [jax.ShapeDtypeStruct((own_pairs, width, width), jnp.float32)]
        out_specs = [inside]
    if after:
        out_shape.append(jax.ShapeDtypeStruct((own_pairs * after, 2, width // 2, width), jnp.bfloat16))
        out_specs.append(inside)
    group = max(g for g in (1, 2, 3, 4, 5) if size % g == 0)
    rounds = units // group
    scratch = [
        pltpu.SMEM(slots.shape, slots.dtype),
        pltpu.SMEM(weights.shape, weights.dtype),
        pltpu.SMEM(info.shape, info.dtype),
        pltpu.SemaphoreType.DMA((3,)),
        pltpu.VMEM((rounds, group, 2, width // 2, width), jnp.bfloat16),
        pltpu.VMEM((rounds, group, ways, share, width), jnp.bfloat16),
        pltpu.VMEM((group, ways, share, width), jnp.bfloat16),
        pltpu.SemaphoreType.DMA((rounds,)),
        pltpu.SemaphoreType.DMA((rounds,)),
    ]
    if after:
        scratch.append(pltpu.SemaphoreType.DMA)
    pair_sems = pltpu.SemaphoreType.DMA((own_pairs,))
    if first:
        scratch += [
            pltpu.VMEM((own_pairs, ways, share, width), jnp.bfloat16),
            pltpu.VMEM((own_pairs, 2, width // 2, width), jnp.bfloat16),
            pltpu.VMEM((own_pairs, width, width), jnp.bfloat16),
            pair_sems, pair_sems, pair_sems,
        ]
    else:
        scratch += [pltpu.VMEM((own_pairs, width, width), jnp.float32), pair_sems]
    stride = slots.shape[0] // own_pairs
    return pl.pallas_call(
        functools.partial(
            coupled_kernel, first, last, size, after, start, stride,
            tuple(o for _, o in got), own_pairs),
        out_shape=out_shape,
        in_specs=[anywhere] * len(operands),
        out_specs=out_specs,
        scratch_shapes=scratch,
        cost_estimate=pl.CostEstimate(
            flops=units * 4 * width**3, bytes_accessed=units * 4 * width**2, transcendentals=0),
        compiler_params=pltpu.CompilerParams(vmem_limit_bytes=VMEM_LIMIT),
        name="coupled",
    )(*operands)


def gather_pairs(half, count):
    me = lax.axis_index("pairs")
    if count > RING_MAX or count % 2:
        return lax.all_gather(half, "pairs", axis=0, tiled=True), lambda block: block
    order = list(range(0, count, 2)) + list(range(count - 1, 0, -2))
    ahead = [(order[i], order[(i + 1) % count]) for i in range(count)]
    behind = [(b, a) for a, b in ahead]
    mid = half.shape[0] // 2
    forward = backward = half
    from_ahead, from_behind = [], []
    for _ in range(1, count // 2):
        forward = lax.ppermute(forward, "pairs", ahead)
        backward = lax.ppermute(backward, "pairs", behind)
        from_behind.append(forward)
        from_ahead.append(backward)
    low = lax.ppermute(forward[:mid], "pairs", ahead)
    high = lax.ppermute(backward[mid:], "pairs", behind)
    whole = jnp.concatenate([half] + from_ahead + [low, high] + from_behind[::-1], axis=0)

    def place_of(block):
        return jnp.where(block % 2 == 0, block // 2, count - 1 - block // 2)

    return whole, lambda block: (place_of(block) - place_of(me) + count) % count


def chunk_bounds(length):
    cuts = [0] + [length * c // 32 for c in CHUNKS] + [length]
    return list(zip(cuts, cuts[1:]))


def shards(
    columns, amplitudes, pno_counts, fock_blocks, exchange_blocks, intersections, partners, couplings
):
    local_pairs, share, width = amplitudes.shape
    ways, count = columns, lax.axis_size("pairs")
    slots_per_pair = partners.shape[1]
    own_pairs = local_pairs // ways
    column = lax.axis_index("cols")

    def swap(array, k):
        return lax.ppermute(array, "cols", [(c, c ^ k) for c in range(ways)])

    col_keep = jnp.arange(width, dtype=jnp.int32)[None, :] < pno_counts[:, None]

    def masked(array, k):
        row = (column ^ k) * share + jnp.arange(share, dtype=jnp.int32)
        keep = (row[None, :] < pno_counts[:, None])[:, :, None] & col_keep[:, None, :]
        return jnp.where(keep, array, jnp.zeros_like(array))

    parts = [masked(amplitudes, 0)]
    parts += [masked(swap(amplitudes, k), k) for k in range(2, ways, 2)]
    half = jnp.concatenate(parts, axis=1)
    bounds = chunk_bounds(slots_per_pair)

    def moved(k, start, stop):
        begin = (column ^ k) * own_pairs
        piece = lax.dynamic_slice(
            intersections, (begin, start, 0, 0), (own_pairs, stop - start, share, width))
        if start == 0:
            extra = lax.dynamic_slice_in_dim(exchange_blocks, begin, own_pairs, 0)
            piece = jnp.concatenate([piece, extra[:, None]], axis=1)
        return swap(piece, k)

    beside = moved(1, 0, slots_per_pair)
    got = []
    for start, stop in bounds:
        got.append([(beside, start)] + [
            (moved(k, start, stop), 0) for k in range(2, ways)])

    near, place = gather_pairs(half, count)
    far = swap(near, 1)

    begin = column * own_pairs
    own_partners = lax.dynamic_slice_in_dim(partners, begin, own_pairs, 0)
    weights = lax.dynamic_slice_in_dim(couplings, begin, own_pairs, 0)
    slots = place(own_partners // local_pairs) * local_pairs + own_partners % local_pairs
    own_counts = lax.dynamic_slice_in_dim(pno_counts, begin, own_pairs, 0)
    own_slots = place(lax.axis_index("pairs")) * local_pairs + begin + jnp.arange(own_pairs, dtype=jnp.int32)
    blocks = column ^ jnp.arange(ways, dtype=jnp.int32)
    info = jnp.concatenate([own_counts, own_slots])

    acc = ready_left = None
    for n, (start, stop) in enumerate(bounds):
        first, last = n == 0, n == len(bounds) - 1
        after = bounds[n + 1][1] - stop if n == len(bounds) - 2 else 0
        outs = run_chunk(
            start, stop - start, after, first, last, ready_left, near, far, intersections,
            got[n], slots.reshape(-1), weights.reshape(-1), info, acc, exchange_blocks, fock_blocks)
        acc = outs if last else outs[0]
        ready_left = outs[1] if after else None
    arrived = [acc[0]] + [swap(acc[k], k) for k in range(1, ways)]
    spots = blocks[:, None, None, None]
    shared = arrived[0][None]
    for k in range(1, ways):
        shared = jnp.where(spots == k, arrived[k][None], shared)
    return shared.reshape(local_pairs, share, width)


def solution(mesh):
    in_specs = (
        P("pairs", "cols", None),
        P("pairs"),
        P("pairs", None, None),
        P("pairs", "cols", None),
        P("pairs", None, "cols", None),
        P("pairs", None),
        P("pairs", None),
    )
    out_specs = P("pairs", "cols", None)
    ways = mesh.shape["cols"]
    body = functools.partial(shards, ways)
    return jax.shard_map(body, mesh=mesh, in_specs=in_specs, out_specs=out_specs, check_vma=False)
```

```python
import functools
import jax
import jax.numpy as jnp
from jax import lax
from jax.experimental import pallas as pl
from jax.experimental.pallas import tpu as pltpu
from jax.sharding import PartitionSpec as P

CHUNKS = (20, 28)
RING_MAX = 8
VMEM_LIMIT = 60 * 2**20


def coupled_kernel(
    taken, first, last, size, after, start, stride, offsets, own_pairs, base_pair, pairs_here,
    slots, weights, info, near, far, own, *refs,
):
    refs = list(refs)
    ways = len(offsets) + 1
    got = [refs.pop(0) for _ in range(ways - 1)]
    if first:
        exch, fock = refs.pop(0), refs.pop(0)
    else:
        acc = refs.pop(0)
    ready_left = refs.pop(0) if taken else None
    outs = [refs.pop(0) for _ in range(ways if last else 1)]
    ahead = refs.pop(0) if after else None
    slot_ref, weight_ref, info_ref, scalar_sem = (refs.pop(0) for _ in range(4))
    left, right, proj, left_sem, right_sem = (refs.pop(0) for _ in range(5))
    ahead_sem = refs.pop(0) if after else None
    group, share, width = right.shape[1], right.shape[3], right.shape[4]
    order = list(range(0, ways, 2)) + list(range(1, ways, 2))
    rounds = size // group
    column = lax.axis_index("cols")
    scalars = [
        pltpu.make_async_copy(source, target, scalar_sem.at[i])
        for i, (source, target) in enumerate(
            ((slots, slot_ref), (weights, weight_ref), (info, info_ref)))
    ]
    for copy in scalars:
        copy.start()

    def block(k):
        return column ^ k

    def fetch_partner(slot, place, sem):
        pltpu.make_async_copy(near.at[slot], place.at[0], sem).start()
        pltpu.make_async_copy(far.at[slot], place.at[1], sem).start()

    def fetch_pieces(r, _):
        m, q = lax.div(r, rounds), lax.rem(r, rounds) * group
        pltpu.make_async_copy(
            own.at[column * own_pairs + base_pair + m, pl.ds(start + q, group)],
            right.at[r, :, block(0)], right_sem.at[r]).start()
        for k in range(1, ways):
            pltpu.make_async_copy(
                got[k - 1].at[offsets[k - 1][0] + m, pl.ds(offsets[k - 1][1] + q, group)],
                right.at[r, :, block(k)], right_sem.at[r]).start()
        if taken:
            pltpu.make_async_copy(
                ready_left.at[pl.ds(r * group, group)], left.at[r], left_sem.at[r]).start()
        return 0

    def fetch_partners(r):
        m, q = lax.div(r, rounds), lax.rem(r, rounds) * group
        for g in range(group):
            fetch_partner(slot_ref[(base_pair + m) * stride + start + q + g], left.at[r, g], left_sem.at[r])
        return 0

    if first:
        base, mine, whole, base_sem, mine_sem, whole_sem = refs
        for m in range(own_pairs):
            pltpu.make_async_copy(
                fock.at[column * own_pairs + m], whole.at[m], whole_sem.at[m]).start()
            pltpu.make_async_copy(
                exch.at[column * own_pairs + m], base.at[m, block(0)], base_sem.at[m]).start()
            for k in range(1, ways):
                pltpu.make_async_copy(
                    got[k - 1].at[m, got[k - 1].shape[1] - 1], base.at[m, block(k)], base_sem.at[m]
                ).start()
    else:
        whole, whole_sem = refs
        for m in range(pairs_here):
            pltpu.make_async_copy(acc.at[base_pair + m], whole.at[m], whole_sem.at[m]).start()

    def fetch(r, _):
        fetch_pieces(r, 0)
        return fetch_partners(r)

    if taken:
        lax.fori_loop(0, pairs_here * rounds, fetch_pieces, 0)
    for copy in scalars:
        copy.wait()
    if first:
        for m in range(own_pairs):
            fetch_partner(info_ref[own_pairs + m], mine.at[m], mine_sem.at[m])
    if not taken:
        lax.fori_loop(0, pairs_here * rounds, fetch, 0)
    for u in range(after):
        fetch_partner(
            slot_ref[(base_pair + 1) * stride + start + u], ahead.at[u], ahead_sem)

    def ready(ref, sem, i):
        pltpu.make_async_copy(ref.at[i], ref.at[i], sem.at[i]).wait()

    def arranged(rows, g):
        for n, k in enumerate(order):
            proj[g, block(k)] = rows[n * share:(n + 1) * share]

    for m in range(pairs_here):
        ready(whole, whole_sem, m)
        total = whole if last else outs[0]
        if first:
            ready(mine, mine_sem, m)
            ready(base, base_sem, m)
            arranged(mine[m].reshape(width, width), 0)
            diagonal = whole[m]
            block_own = proj[0].reshape(width, width)
            sums = base[m].reshape(width, width).astype(jnp.float32)
            sums = sums + jnp.dot(diagonal, block_own, preferred_element_type=jnp.float32)
            total[m] = sums + jnp.dot(block_own, diagonal, preferred_element_type=jnp.float32)
        elif not last:
            total[m] = whole[m]

        def body(n, _):
            r = m * rounds + n
            ready(left, left_sem, r)
            ready(right, right_sem, r)
            for g in range(group):
                prod = jnp.dot(
                    left[r, g].reshape(width, width), right[r, g].reshape(width, width),
                    preferred_element_type=jnp.float32)
                arranged(prod.astype(jnp.bfloat16), g)
            added = None
            for g in range(group):
                term = lax.dot_general(
                    right[r, g].reshape(width, width), proj[g].reshape(width, width),
                    (((0,), (0,)), ((), ())), preferred_element_type=jnp.float32)
                term = weight_ref[(base_pair + m) * stride + start + n * group + g] * term
                added = term if added is None else added + term
            total[m] = total[m] + added
            return 0

        lax.fori_loop(0, rounds, body, 0)
        if last:
            count = info_ref[base_pair + m]
            row = lax.broadcasted_iota(jnp.int32, (width, width), 0)
            col = lax.broadcasted_iota(jnp.int32, (width, width), 1)
            keep = (row < count) & (col < count)
            total[m] = jnp.where(keep, total[m], 0.0)
            for k in range(ways):
                rows = pl.ds(pl.multiple_of(block(k) * share, share), share)
                outs[k][m] = total[m, rows, :].astype(jnp.bfloat16)
    if after:
        pltpu.make_async_copy(ahead, ahead, ahead_sem).wait()


def run_chunk(
    start, size, base_pair, pairs_here, after, first, last, ready_left, near, far, own_pieces, got, slots, weights, info, acc, exch, fock
):
    own_pairs = got[0][0].shape[0]
    taken = ready_left is not None
    ways = len(got) + 1
    width = near.shape[2]
    share = own_pieces.shape[2]
    units = pairs_here * size
    anywhere = pl.BlockSpec(memory_space=pl.ANY)
    operands = [slots, weights, info, near, far, own_pieces] + [piece for piece, _ in got]
    operands += [exch, fock] if first else [acc]
    if taken:
        operands.append(ready_left)
    inside = pl.BlockSpec(memory_space=pltpu.VMEM)
    if last:
        out_shape = [jax.ShapeDtypeStruct((pairs_here, share, width), jnp.bfloat16)] * ways
        out_specs = [inside] * ways
    else:
        out_shape = [jax.ShapeDtypeStruct((own_pairs, width, width), jnp.float32)]
        out_specs = [inside]
    if after:
        out_shape.append(jax.ShapeDtypeStruct((after, 2, width // 2, width), jnp.bfloat16))
        out_specs.append(inside)
    group = max(g for g in (1, 2, 3, 4, 5) if size % g == 0)
    rounds = units // group
    scratch = [
        pltpu.SMEM(slots.shape, slots.dtype),
        pltpu.SMEM(weights.shape, weights.dtype),
        pltpu.SMEM(info.shape, info.dtype),
        pltpu.SemaphoreType.DMA((3,)),
        pltpu.VMEM((rounds, group, 2, width // 2, width), jnp.bfloat16),
        pltpu.VMEM((rounds, group, ways, share, width), jnp.bfloat16),
        pltpu.VMEM((group, ways, share, width), jnp.bfloat16),
        pltpu.SemaphoreType.DMA((rounds,)),
        pltpu.SemaphoreType.DMA((rounds,)),
    ]
    if after:
        scratch.append(pltpu.SemaphoreType.DMA)
    pair_sems = pltpu.SemaphoreType.DMA((own_pairs,))
    if first:
        scratch += [
            pltpu.VMEM((own_pairs, ways, share, width), jnp.bfloat16),
            pltpu.VMEM((own_pairs, 2, width // 2, width), jnp.bfloat16),
            pltpu.VMEM((own_pairs, width, width), jnp.bfloat16),
            pair_sems, pair_sems, pair_sems,
        ]
    else:
        scratch += [pltpu.VMEM((pairs_here, width, width), jnp.float32), pair_sems]
    stride = slots.shape[0] // own_pairs
    return pl.pallas_call(
        functools.partial(
            coupled_kernel, taken, first, last, size, after, start, stride,
            tuple(o for _, o in got), own_pairs, base_pair, pairs_here),
        out_shape=out_shape,
        in_specs=[anywhere] * len(operands),
        out_specs=out_specs,
        scratch_shapes=scratch,
        cost_estimate=pl.CostEstimate(
            flops=units * 4 * width**3, bytes_accessed=units * 4 * width**2, transcendentals=0),
        compiler_params=pltpu.CompilerParams(vmem_limit_bytes=VMEM_LIMIT),
        name="coupled",
    )(*operands)


def gather_pairs(half, count):
    me = lax.axis_index("pairs")
    if count > RING_MAX or count % 2:
        return lax.all_gather(half, "pairs", axis=0, tiled=True), lambda block: block
    order = list(range(0, count, 2)) + list(range(count - 1, 0, -2))
    ahead = [(order[i], order[(i + 1) % count]) for i in range(count)]
    behind = [(b, a) for a, b in ahead]
    mid = half.shape[0] // 2
    forward = backward = half
    from_ahead, from_behind = [], []
    for _ in range(1, count // 2):
        forward = lax.ppermute(forward, "pairs", ahead)
        backward = lax.ppermute(backward, "pairs", behind)
        from_behind.append(forward)
        from_ahead.append(backward)
    low = lax.ppermute(forward[:mid], "pairs", ahead)
    high = lax.ppermute(backward[mid:], "pairs", behind)
    whole = jnp.concatenate([half] + from_ahead + [low, high] + from_behind[::-1], axis=0)

    def place_of(block):
        return jnp.where(block % 2 == 0, block // 2, count - 1 - block // 2)

    return whole, lambda block: (place_of(block) - place_of(me) + count) % count


def chunk_bounds(length, own_pairs):
    cuts = [0] + [length * c // 32 for c in CHUNKS]
    together = [(0, own_pairs, *cut) for cut in zip(cuts, cuts[1:])]
    return together + [(m, m + 1, cuts[-1], length) for m in range(own_pairs)]


def shards(
    columns, amplitudes, pno_counts, fock_blocks, exchange_blocks, intersections, partners, couplings
):
    local_pairs, share, width = amplitudes.shape
    ways, count = columns, lax.axis_size("pairs")
    slots_per_pair = partners.shape[1]
    own_pairs = local_pairs // ways
    column = lax.axis_index("cols")

    def swap(array, k):
        return lax.ppermute(array, "cols", [(c, c ^ k) for c in range(ways)])

    col_keep = jnp.arange(width, dtype=jnp.int32)[None, :] < pno_counts[:, None]

    def masked(array, k):
        row = (column ^ k) * share + jnp.arange(share, dtype=jnp.int32)
        keep = (row[None, :] < pno_counts[:, None])[:, :, None] & col_keep[:, None, :]
        return jnp.where(keep, array, jnp.zeros_like(array))

    parts = [masked(amplitudes, 0)]
    parts += [masked(swap(amplitudes, k), k) for k in range(2, ways, 2)]
    half = jnp.concatenate(parts, axis=1)
    bounds = chunk_bounds(slots_per_pair, own_pairs)

    def moved(k, low, high, start, stop):
        begin = (column ^ k) * own_pairs
        piece = lax.dynamic_slice(
            intersections, (begin + low, start, 0, 0), (high - low, stop - start, share, width))
        if start == 0:
            extra = lax.dynamic_slice_in_dim(exchange_blocks, begin, own_pairs, 0)
            piece = jnp.concatenate([piece, extra[:, None]], axis=1)
        return swap(piece, k)

    beside = moved(1, 0, own_pairs, 0, slots_per_pair)
    got = []
    for low, high, start, stop in bounds:
        got.append([(beside, (low, start))] + [
            (moved(k, low, high, start, stop), (0, 0)) for k in range(2, ways)])

    near, place = gather_pairs(half, count)
    far = swap(near, 1)

    begin = column * own_pairs
    own_partners = lax.dynamic_slice_in_dim(partners, begin, own_pairs, 0)
    weights = lax.dynamic_slice_in_dim(couplings, begin, own_pairs, 0)
    slots = place(own_partners // local_pairs) * local_pairs + own_partners % local_pairs
    own_counts = lax.dynamic_slice_in_dim(pno_counts, begin, own_pairs, 0)
    own_slots = place(lax.axis_index("pairs")) * local_pairs + begin + jnp.arange(own_pairs, dtype=jnp.int32)
    blocks = column ^ jnp.arange(ways, dtype=jnp.int32)
    info = jnp.concatenate([own_counts, own_slots])

    acc = ready_left = None
    arrived = [[] for _ in range(ways)]
    for n, (low, high, start, stop) in enumerate(bounds):
        last = n >= len(CHUNKS)
        after = stop - start if last and high < own_pairs else 0
        outs = run_chunk(
            start, stop - start, low, high - low, after, n == 0, last, ready_left, near, far,
            intersections, got[n], slots.reshape(-1), weights.reshape(-1), info, acc,
            exchange_blocks, fock_blocks)
        ready_left = outs[-1] if after else None
        if last:
            for k in range(ways):
                arrived[k].append(outs[k] if k == 0 else swap(outs[k], k))
        else:
            acc = outs[0]
    arrived = [jnp.concatenate(parts) for parts in arrived]
    spots = blocks[:, None, None, None]
    shared = arrived[0][None]
    for k in range(1, ways):
        shared = jnp.where(spots == k, arrived[k][None], shared)
    return shared.reshape(local_pairs, share, width)


def solution(mesh):
    in_specs = (
        P("pairs", "cols", None),
        P("pairs"),
        P("pairs", None, None),
        P("pairs", "cols", None),
        P("pairs", None, "cols", None),
        P("pairs", None),
        P("pairs", None),
    )
    out_specs = P("pairs", "cols", None)
    ways = mesh.shape["cols"]
    body = functools.partial(shards, ways)
    return jax.shard_map(body, mesh=mesh, in_specs=in_specs, out_specs=out_specs, check_vma=False)
```
